32 devices in a mesh: grp: 2 (over x), tok: 8 (over z, y), mdl: 2 (over core).
Axes of the slice: x: 2, y: 2, z: 4, core: 2. Of those that a mesh axis runs over, the one named last changes fastest.
Arguments:
- hidden: bfloat16 [1024, 4096], P(('grp', 'tok'), 'mdl'), parts along dimension 0, may hold values from -3 to 3
- queries: bfloat16 [1024, 16, 128], P(('grp', 'tok'), 'mdl'), parts along dimension 0, may hold values from -8 to 8
- cache: bfloat16 [16, 2048, 4, 2, 128], P(('grp', 'tok'), None, 'mdl'), parts along dimension 0, may hold values from -8 to 8
- cache_lengths: int32 [16], P(('grp', 'tok')), parts along dimension 0, may hold values from 128 to 2048, as said below
- wkv: bfloat16 [4096, 4, 2, 128], P('tok', 'mdl'), may hold values from -0.09375 to 0.09375
- wo: bfloat16 [16, 128, 4096], P('mdl', None, 'tok'), may hold values from -0.5 to 0.5
- attn_gain: bfloat16 [4096], replicated, may hold values from 0.5 to 1.5
- moe_gain: bfloat16 [4096], replicated, may hold values from 0.5 to 1.5
- w_gate: bfloat16 [16, 4096, 1792], P(('tok', 'mdl')), may hold values from -0.09375 to 0.09375
- w_up: bfloat16 [16, 4096, 1792], P(('tok', 'mdl')), may hold values from -0.09375 to 0.09375
- w_down: bfloat16 [16, 1792, 4096], P(('tok', 'mdl')), may hold values from -0.0625 to 0.0625
- expert_ids: int32 [1024, 2], P(('grp', 'tok', 'mdl')), parts along dimension 0, may hold values from 0 to 3, all different within a row; in each aligned block of 32 rows (0 to 31, 32 to 63, ...) at most 18 rows name the same one
- gates: float32 [1024, 2], P(('grp', 'tok', 'mdl')), parts along dimension 0, may hold values from 0.1 to 1
Outputs:
- mixed: bfloat16 [1024, 4096], P(('grp', 'tok', 'mdl')), parts along dimension 0
- fresh_key_value: bfloat16 [1024, 4, 2, 128], P(('grp', 'tok'), 'mdl'), parts along dimension 0
The draws below stay inside these ranges and needn't reach their ends.
There are 2 independent parts, one for each index of `grp`. The reference program is written for one: setup_inputs(seed, part) draws one part's arguments, and reference() takes and returns one part's arrays. A program takes and returns all parts, laid end to end along the dimension named above; an argument that names none is the same for every part. Nothing has to cross between parts.
Inputs may be any that keep to these rules, and one draw needn't show every extreme that they name: `expert_ids`: each token names 2 different experts; in aligned blocks of 32 rows no expert is named by more than 18 rows, a bound that some block reaches. `cache_lengths`: some rollout holds exactly 2048 cached positions.
All inputs are finite; a program needn't handle non-finite values.
Results may differ from the reference program's by a relative error of at most 0.007.
Values may be sent and summed in bfloat16 or wider, within the bound.
A program may use at most 128 MiB of HBM per device.

```python
import math
import jax
import jax.numpy as jnp
import numpy as np
from jax import lax

MODEL_DIM = 4096
HEAD_SIZE = 128
QUERY_HEADS = 16
KEY_VALUE_HEADS = 4
EXPERTS = 4
FF = 7168
TOPK = 2
NEW_TOKEN_SPAN = 64
CACHE_LIMIT = 2048
ROLLOUT_COUNT = 8
TOKEN_TOTAL = 512
TOK_MOE = 32
CAP = 18
SLABS = 4
FS = 1792
N_TOK = 8
N_MDL = 2


def draw_queries(key, part):
    array_shape = (TOKEN_TOTAL, QUERY_HEADS, HEAD_SIZE)
    return jnp.clip(jax.random.normal(jax.random.fold_in(key, 1), array_shape, jnp.float32) * 2.5, -7.5, 7.5).astype(jnp.bfloat16)


def draw_cache(key, part):
    array_shape = (ROLLOUT_COUNT, CACHE_LIMIT, KEY_VALUE_HEADS, 2, HEAD_SIZE)
    return jnp.clip(jax.random.normal(jax.random.fold_in(key, 2), array_shape, jnp.float32), -5.0, 5.0).astype(jnp.bfloat16)


def draw_cache_lengths(key, part):
    values = jax.random.randint(jax.random.fold_in(key, 3), (ROLLOUT_COUNT,), CACHE_LIMIT // 16, CACHE_LIMIT + 1)
    longest = jax.random.randint(jax.random.fold_in(key, 4), (), 0, ROLLOUT_COUNT)
    return jnp.where(jnp.arange(ROLLOUT_COUNT) == longest, CACHE_LIMIT, values).astype(jnp.int32)


def block_scale(stream_key, dims, split, smallest, top_value):
    level = 1.0
    for position, shards_of in split:
        steps = jax.random.uniform(jax.random.fold_in(jax.random.fold_in(stream_key, 6), position), (shards_of,), jnp.float32, smallest / len(split), top_value / len(split))
        level = level * jnp.repeat(jnp.exp(steps), dims[position] // shards_of).reshape((-1,) + (1,) * (len(dims) - 1 - position))
    return level


def routed_block(stream_key, own, number, rows, count, top, most, slope):
    ranking = jax.random.permutation(stream_key, count)
    crowded, usual = load_shares(count, rows * top, most, slope, True), load_shares(count, rows * top, most, slope, False)
    places = jnp.arange(count)

    def named(tallies, rotation):
        used = int((tallies > 0).sum())
        fixed = max(1, used // 4)
        shifted = fixed + (places - fixed + rotation * (used - fixed)) % max(1, count - fixed)
        return jnp.zeros((count,), jnp.int32).at[ranking[jnp.where(places < fixed, places, shifted)]].set(jnp.asarray(tallies, jnp.int32))

    tallies = jnp.where(number % 4 == 0, named(crowded, number // 4), named(usual, number - number // 4 - 1))
    mixed = jax.random.permutation(jax.random.fold_in(own, 3), count)
    source_of, receiver = mixed[0:count // 2 * 2:2], mixed[1:count // 2 * 2:2]
    room = jnp.minimum(tallies[source_of] - 1, most - tallies[receiver]) // 2
    room = jnp.where((source_of == ranking[0]) | (receiver == ranking[0]) | (tallies[receiver] == 0), 0, jnp.maximum(room, 0))
    shifted = jax.random.randint(jax.random.fold_in(own, 4), (count // 2,), 0, 1 << 20) % (room + 1)
    tallies = tallies.at[source_of].add(-shifted).at[receiver].add(shifted)
    items = jnp.searchsorted(jnp.cumsum(tallies), jnp.arange(rows * top), side="right").astype(jnp.int32)
    grid = items.reshape(top, rows).T
    grid = grid[jax.random.permutation(jax.random.fold_in(own, 1), rows)]
    rotation = jax.random.randint(jax.random.fold_in(own, 2), (rows, 1), 0, top)
    return jnp.take_along_axis(grid, (jnp.arange(top)[None, :] + rotation) % top, axis=1)


def load_shares(amount, total, reach, skew, full):
    weights = [(1 << 20) // math.isqrt(rank ** skew) + 1 for rank in range(1, amount + 1)]
    largest = reach if full else min(reach, max(-(-total // amount), total * weights[0] // sum(weights)))
    least = 1 if total - largest >= amount - 1 else 0
    holding, surplus = [largest] + [least] * (amount - 1), total - largest - least * (amount - 1)
    while surplus > 0:
        candidates = [i for i in range(1, amount) if holding[i] < largest] or [i for i in range(1, amount) if holding[i] < reach]
        whole, left = sum([weights[i] for i in candidates]), surplus
        for i in candidates:
            extra = min(reach - holding[i], max(1, left * weights[i] // whole), surplus)
            holding[i] = holding[i] + extra
            surplus = surplus - extra
    return np.array(holding)


def bell_draw(rng, shape, width, most, split=(), kind=jnp.bfloat16):
    drawn = width * jax.random.normal(rng, shape, jnp.float32)
    if split:
        drawn = drawn * block_scale(rng, shape, split, -0.22, 0.18)
    return jnp.clip(drawn, -most, most).astype(kind)


def setup_inputs(seed: int = 0, part: int = 0) -> dict:
    key_of = jax.random.split(jax.random.key(seed), 14)
    part_keys = jax.random.split(jax.random.fold_in(key_of[13], part), 14)
    hidden = bell_draw(part_keys[0], (TOKEN_TOTAL, MODEL_DIM), 0.5, 3.0, ((0, 8), (1, 2)))
    queries = draw_queries(jax.random.fold_in(jax.random.fold_in(key_of[13], part), 71), part)
    cache = draw_cache(jax.random.fold_in(jax.random.fold_in(key_of[13], part), 71), part)
    cache_lengths = draw_cache_lengths(jax.random.fold_in(jax.random.fold_in(key_of[13], part), 71), part)
    wkv = bell_draw(key_of[4], (MODEL_DIM, KEY_VALUE_HEADS, 2, HEAD_SIZE), MODEL_DIM ** -0.5, 0.09375, ((0, 8), (1, 2)))
    wo = bell_draw(key_of[5], (QUERY_HEADS, HEAD_SIZE, MODEL_DIM), HEAD_SIZE ** -0.5, 0.5, ((0, 2), (2, 8)))
    attn_gain = jnp.clip(1.0 + 0.1 * jax.random.normal(key_of[6], (MODEL_DIM,), jnp.float32), 0.5, 1.5).astype(jnp.bfloat16)
    moe_gain = jnp.clip(1.0 + 0.1 * jax.random.normal(key_of[7], (MODEL_DIM,), jnp.float32), 0.5, 1.5).astype(jnp.bfloat16)
    w_gate = bell_draw(key_of[8], (EXPERTS * SLABS, MODEL_DIM, FS), MODEL_DIM ** -0.5, 0.09375, ((0, 16),))
    w_up = bell_draw(key_of[9], (EXPERTS * SLABS, MODEL_DIM, FS), MODEL_DIM ** -0.5, 0.09375, ((0, 16),))
    w_down = bell_draw(key_of[10], (EXPERTS * SLABS, FS, MODEL_DIM), FF ** -0.5, 0.0625, ((0, 16),))
    expert_ids_keys = jax.random.split(jax.random.fold_in(part_keys[11], 1), TOKEN_TOTAL // TOK_MOE)
    expert_ids_turns = jax.random.permutation(jax.random.fold_in(part_keys[11], 3), TOKEN_TOTAL // TOK_MOE)
    expert_ids = jax.vmap(lambda own, number: routed_block(jax.random.fold_in(part_keys[11], 2), own, number, TOK_MOE, EXPERTS, TOPK, CAP, 2))(expert_ids_keys, expert_ids_turns).reshape((TOKEN_TOTAL, TOPK))
    gates = jnp.clip(0.1 + 0.9 * jax.random.uniform(part_keys[12], (TOKEN_TOTAL, TOPK), jnp.float32) ** block_scale(part_keys[12], (TOKEN_TOTAL, TOPK), ((0, 16),), -0.2, 0.2), 0.1, 1.0)
    return dict(hidden=hidden, queries=queries, cache=cache, cache_lengths=cache_lengths, wkv=wkv, wo=wo, attn_gain=attn_gain, moe_gain=moe_gain, w_gate=w_gate, w_up=w_up, w_down=w_down, expert_ids=expert_ids, gates=gates)


eps_norm = 1e-05
rope_base = 1000000.0
mask_fill = -1e+30

def rms_scale(values_in, gain):
    values = values_in.astype(jnp.float32)
    meansq = lax.optimization_barrier(jnp.mean(values * values, axis=-1, keepdims=True))
    return values * lax.rsqrt(meansq + eps_norm) * gain.astype(jnp.float32)

def rotate(key_rows, positions):
    half_dim = key_rows.shape[-1] // 2
    inverse = jnp.exp(jnp.arange(half_dim, dtype=jnp.float32) * (-2.0 * math.log(rope_base) / key_rows.shape[-1]))
    angle = positions.astype(jnp.float32)[:, None] * inverse[None, :]
    cosine = jnp.cos(angle)[:, None, :]
    sine_vals = jnp.sin(angle)[:, None, :]
    front_half = key_rows[..., :half_dim]
    back_half = key_rows[..., half_dim:]
    return jnp.concatenate([front_half * cosine - back_half * sine_vals, back_half * cosine + front_half * sine_vals], axis=-1)

def reference(hidden, queries, cache, cache_lengths, wkv, wo, attn_gain, moe_gain, w_gate, w_up, w_down, expert_ids, gates):
    normalized_input = rms_scale(hidden, attn_gain).astype(jnp.bfloat16)
    key_value_projection = jnp.dot(normalized_input, wkv.reshape(MODEL_DIM, KEY_VALUE_HEADS * 2 * HEAD_SIZE), preferred_element_type=jnp.float32).reshape(TOKEN_TOTAL, KEY_VALUE_HEADS, 2, HEAD_SIZE)
    positions = (cache_lengths[:, None] + jnp.arange(NEW_TOKEN_SPAN, dtype=jnp.int32)[None, :]).reshape(TOKEN_TOTAL).astype(jnp.int32)
    fresh_key_value = jnp.stack([rotate(key_value_projection[:, :, 0], positions), key_value_projection[:, :, 1]], axis=2).astype(jnp.bfloat16)
    head_group = QUERY_HEADS // KEY_VALUE_HEADS
    scale_factor = 1.0 / math.sqrt(HEAD_SIZE)
    query_all = queries.reshape(ROLLOUT_COUNT, NEW_TOKEN_SPAN, QUERY_HEADS, HEAD_SIZE)
    fresh_all_rows = fresh_key_value.reshape(ROLLOUT_COUNT, NEW_TOKEN_SPAN, KEY_VALUE_HEADS, 2, HEAD_SIZE)

    def one_rollout(packed):
        query_roll, cache_roll, new_roll, length = packed
        token_of_row = jnp.arange(NEW_TOKEN_SPAN * head_group) // head_group
        column = jnp.arange(CACHE_LIMIT + NEW_TOKEN_SPAN)
        allowed = jnp.where(column[None, :] < CACHE_LIMIT, column[None, :] < length, column[None, :] - CACHE_LIMIT <= token_of_row[:, None])
        outputs = []
        for head_index in range(KEY_VALUE_HEADS):
            query_rows = query_roll[:, head_index * head_group:(head_index + 1) * head_group].reshape(NEW_TOKEN_SPAN * head_group, HEAD_SIZE)
            key_rows = jnp.concatenate([cache_roll[:, head_index, 0], new_roll[:, head_index, 0]], axis=0)
            value_rows = jnp.concatenate([cache_roll[:, head_index, 1], new_roll[:, head_index, 1]], axis=0)
            scores = lax.dot_general(query_rows, key_rows, (((1,), (1,)), ((), ())), preferred_element_type=jnp.float32) * scale_factor
            scores = jnp.where(allowed, scores, mask_fill)
            row_max = lax.optimization_barrier(jnp.max(scores, axis=1, keepdims=True))
            weights = jnp.where(allowed, jnp.exp(scores - row_max), 0.0)
            probs = (weights / lax.optimization_barrier(jnp.sum(weights, axis=1, keepdims=True))).astype(jnp.bfloat16)
            attended = jnp.dot(probs, value_rows, preferred_element_type=jnp.float32).astype(jnp.bfloat16)
            outputs.append(attended.reshape(NEW_TOKEN_SPAN, head_group * HEAD_SIZE))
        return jnp.concatenate(outputs, axis=1)
    heads_out = lax.map(one_rollout, (query_all, cache, fresh_all_rows, cache_lengths)).reshape(TOKEN_TOTAL, QUERY_HEADS * HEAD_SIZE)
    attn_out = jnp.dot(heads_out, wo.reshape(QUERY_HEADS * HEAD_SIZE, MODEL_DIM), preferred_element_type=jnp.float32)
    resid = hidden.astype(jnp.float32) + attn_out
    moe_in = rms_scale(resid, moe_gain).astype(jnp.bfloat16)
    limit = N_TOK * N_MDL * CAP
    moe_out = jnp.zeros((TOKEN_TOTAL, MODEL_DIM), jnp.float32)
    for expert_idx in range(EXPERTS):
        match = expert_ids == expert_idx
        routed = jnp.any(match, axis=1)
        weight = lax.optimization_barrier(jnp.sum(jnp.where(match, gates, 0.0), axis=1)).astype(jnp.float32)
        order = jnp.argsort(jnp.where(routed, 0, 1).astype(jnp.int32), stable=True)[:limit].astype(jnp.int32)
        rows_in = moe_in[order]

        def slab_step(total, slab_idx):
            row_idx = expert_idx * SLABS + slab_idx
            gate_w = lax.dynamic_index_in_dim(w_gate, row_idx, 0, keepdims=False)
            up_w = lax.dynamic_index_in_dim(w_up, row_idx, 0, keepdims=False)
            down_w = lax.dynamic_index_in_dim(w_down, row_idx, 0, keepdims=False)
            gate_val = jnp.dot(rows_in, gate_w, preferred_element_type=jnp.float32)
            up_val = jnp.dot(rows_in, up_w, preferred_element_type=jnp.float32)
            slab_hidden = (jax.nn.silu(gate_val) * up_val).astype(jnp.bfloat16)
            slab_out = jnp.dot(slab_hidden, down_w, preferred_element_type=jnp.float32).astype(jnp.bfloat16)
            return (total + slab_out.astype(jnp.float32), None)
        total, unused = lax.scan(slab_step, jnp.zeros((limit, MODEL_DIM), jnp.float32), jnp.arange(SLABS, dtype=jnp.int32))
        moe_out = moe_out.at[order].add(weight[order][:, None] * total)
    mixed = (resid + moe_out).astype(jnp.bfloat16)
    return (mixed, fresh_key_value)
```

```python
import functools
import math

import jax
import jax.numpy as jnp
from jax import lax
from jax.experimental import pallas as pl
from jax.experimental.pallas import tpu as pltpu
from jax.sharding import PartitionSpec as P

EXPERTS = 4
TOPK = 2


eps_norm = 1e-05
rope_base = 1000000.0
mask_fill = -1e30


def rms_scale(values_in, gain):
    values = values_in.astype(jnp.float32)
    meansq = jnp.mean(values * values, axis=-1, keepdims=True)
    return values * lax.rsqrt(meansq + eps_norm) * gain.astype(jnp.float32)


def rotate(key_rows, positions):
    half_dim = key_rows.shape[-1] // 2
    inverse = jnp.exp(
        jnp.arange(half_dim, dtype=jnp.float32) * (-2.0 * math.log(rope_base) / key_rows.shape[-1])
    )
    angle = positions.astype(jnp.float32)[:, None] * inverse[None, :]
    cosine = jnp.cos(angle)[:, None, :]
    sine_vals = jnp.sin(angle)[:, None, :]
    front_half = key_rows[..., :half_dim]
    back_half = key_rows[..., half_dim:]
    return jnp.concatenate(
        [front_half * cosine - back_half * sine_vals, back_half * cosine + front_half * sine_vals],
        axis=-1,
    )


def score_rows(query_rows, key_rows, scale_factor):
    return (
        lax.dot_general(
            query_rows, key_rows, (((1,), (1,)), ((), ())), preferred_element_type=jnp.float32
        )
        * scale_factor
    )


def head_attention(query_rows, cache_keys, cache_values, length, new_keys, new_values, head_group):
    row_count = query_rows.shape[0]
    block_len = min(512, cache_keys.shape[0])
    scale_factor = 1.0 / math.sqrt(query_rows.shape[1])
    token_of_row = jnp.arange(row_count) // head_group
    block_total = (length + block_len - 1) // block_len

    def block_scores(block_idx):
        row_offset = block_idx * block_len
        block_keys = lax.dynamic_slice_in_dim(cache_keys, row_offset, block_len, 0)
        allowed = row_offset + jnp.arange(block_len) < length
        return (
            jnp.where(
                allowed[None, :], score_rows(query_rows, block_keys, scale_factor), mask_fill
            ),
            allowed,
        )

    new_allowed = jnp.arange(new_keys.shape[0])[None, :] <= token_of_row[:, None]
    new_scores = jnp.where(new_allowed, score_rows(query_rows, new_keys, scale_factor), mask_fill)
    first_max = jnp.max(new_scores, axis=1)
    first_sum = jnp.sum(
        jnp.where(new_allowed, jnp.exp(new_scores - first_max[:, None]), 0.0), axis=1
    )

    def first_pass(block_idx, carry):
        run_max, run_sum = carry
        scores, allowed = block_scores(block_idx)
        next_max = jnp.maximum(run_max, jnp.max(scores, axis=1))
        weights = jnp.where(allowed[None, :], jnp.exp(scores - next_max[:, None]), 0.0)
        return (next_max, run_sum * jnp.exp(run_max - next_max) + jnp.sum(weights, axis=1))

    row_max, row_sum = lax.fori_loop(0, block_total, first_pass, (first_max, first_sum))
    new_probs = (
        jnp.where(new_allowed, jnp.exp(new_scores - row_max[:, None]), 0.0) / row_sum[:, None]
    ).astype(jnp.bfloat16)
    start_total = jnp.dot(new_probs, new_values, preferred_element_type=jnp.float32)

    def second_pass(block_idx, total):
        scores, allowed = block_scores(block_idx)
        probs = (
            jnp.where(allowed[None, :], jnp.exp(scores - row_max[:, None]), 0.0) / row_sum[:, None]
        ).astype(jnp.bfloat16)
        block_values = lax.dynamic_slice_in_dim(cache_values, block_idx * block_len, block_len, 0)
        return total + jnp.dot(probs, block_values, preferred_element_type=jnp.float32)

    total = lax.fori_loop(0, block_total, second_pass, start_total)
    return total.astype(jnp.bfloat16)


MESH = pl.DeviceIdType.MESH
VMEM = pl.BlockSpec(memory_space=pltpu.VMEM)


def place(tok, mdl):
    return (lax.axis_index("grp"), tok, mdl)


def greet(peers):
    barrier = pltpu.get_barrier_semaphore()
    for peer in peers:
        pl.semaphore_signal(barrier, inc=1, device_id=peer, device_id_type=MESH)
    pl.semaphore_wait(barrier, len(peers))


def peers_of(groups, ranks, cores):
    tok, mdl = lax.axis_index("tok"), lax.axis_index("mdl")
    group, rank = tok // ranks, tok % ranks
    peers = [place((group + d) % groups * ranks + rank, mdl) for d in range(1, groups)]
    peers += [place(group * ranks + (rank + d) % ranks, mdl) for d in range(1, ranks)]
    if cores:
        peers.append(place(tok, 1 - mdl))
    return peers


def remote(src, dst, sems, index, device):
    copy = pltpu.make_async_remote_copy(
        src_ref=src,
        dst_ref=dst,
        send_sem=sems.at[0, index],
        recv_sem=sems.at[1, index],
        device_id=device,
        device_id_type=MESH,
    )
    copy.start()
    return copy


def spread_kernel(groups, ranks, cores, same, send, out, sems, local_sem):
    tok, mdl = lax.axis_index("tok"), lax.axis_index("mdl")
    group, rank = tok // ranks, tok % ranks
    greet(peers_of(groups, ranks, cores))

    def piece(index):
        return send if same else send.at[index]

    def slot(index):
        return out.at[index, mdl] if cores else out.at[index]

    started = []
    count = [0]

    def go(src, dst, device):
        copy = remote(src, dst, sems, count[0], device)
        count[0] += 1
        started.append(copy)
        return copy

    own = pltpu.make_async_copy(piece(group), slot(tok), local_sem)
    own.start()
    first = {}
    for d in range(1, groups):
        there = (group + d) % groups
        first[d] = go(piece(there), slot(tok), place(there * ranks + rank, mdl))
    second, third = [], []

    def onward(src, index):
        for d in range(1, ranks):
            there = group * ranks + (rank + d) % ranks
            second.append((d, index, go(src, slot(index), place(there, mdl))))

    def across(src, index):
        if cores:
            third.append(go(src, slot(index), place(tok, 1 - mdl)))

    onward(piece(group), tok)
    across(piece(group), tok)
    for d in range(1, groups):
        first[d].wait_recv()
        index = (group + groups - d) % groups * ranks + rank
        onward(slot(index), index)
        across(slot(index), index)
    for d, index, copy in second:
        copy.wait_recv()
        index = index // ranks * ranks + (rank + ranks - d) % ranks
        across(slot(index), index)
    for copy in third:
        copy.wait_recv()
    for copy in started:
        copy.wait_send()
    own.wait()


def spread(send, groups, ranks, cores, same, number):
    tiles = send.shape if same else send.shape[1:]
    toks = groups * ranks
    core_count = lax.axis_size("mdl") if cores else 1
    lead = (toks, core_count) if cores else (toks,)
    copies = groups - 1 + groups * (ranks - 1) + (toks if cores else 0)
    return pl.pallas_call(
        functools.partial(spread_kernel, groups, ranks, cores, same),
        out_shape=jax.ShapeDtypeStruct(lead + tiles, send.dtype),
        in_specs=[VMEM],
        out_specs=VMEM,
        scratch_shapes=[pltpu.SemaphoreType.DMA((2, copies)), pltpu.SemaphoreType.DMA],
        compiler_params=pltpu.CompilerParams(
            collective_id=number, has_side_effects=True, vmem_limit_bytes=40 * 1024 * 1024
        ),
    )(send)


def collect_kernel(groups, ranks, parts, out, near, held, mid, sems):
    tok, mdl = lax.axis_index("tok"), lax.axis_index("mdl")
    group, rank = tok // ranks, tok % ranks
    greet(peers_of(groups, ranks, True))
    started = []
    count = [0]

    def go(src, dst, device):
        copy = remote(src, dst, sems, count[0], device)
        count[0] += 1
        started.append(copy)
        return copy

    order = [
        (r, g)
        for r in list(range(1, ranks)) + [0]
        for g in list(range(1, groups)) + [0]
    ]

    def index_of(r, g):
        return (group + g) % groups * ranks + (rank + r) % ranks

    across = {}
    for r, g in order:
        index = index_of(r, g)
        across[r, g] = go(parts.at[index, 1 - mdl], near.at[index], place(tok, 1 - mdl))
    second = {}
    for r, g in order:
        if r == 0:
            continue
        index = index_of(r, g)
        across[r, g].wait_recv()
        both = parts[index, mdl].astype(jnp.float32) + near[index].astype(jnp.float32)
        held[index] = both.astype(held.dtype)
        second[r, g] = go(
            held.at[index], mid.at[r - 1, g], place(group * ranks + (rank + r) % ranks, mdl)
        )
    last = []
    for g in list(range(1, groups)) + [0]:
        index = index_of(0, g)
        across[0, g].wait_recv()
        total = parts[index, mdl].astype(jnp.float32) + near[index].astype(jnp.float32)
        for r in range(1, ranks):
            second[r, g].wait_recv()
            total = total + mid[r - 1, g].astype(jnp.float32)
        if g == 0:
            out[group] = total.astype(out.dtype)
        else:
            held[index] = total.astype(held.dtype)
            last.append(
                go(held.at[index], out.at[group], place((group + g) % groups * ranks + rank, mdl))
            )
    for copy in last:
        copy.wait_recv()
    for copy in started:
        copy.wait_send()


def collect(parts, groups, ranks, number):
    toks = groups * ranks
    tile = parts.shape[2:]
    copies = toks + groups * (ranks - 1) + groups - 1
    return pl.pallas_call(
        functools.partial(collect_kernel, groups, ranks),
        out_shape=jax.ShapeDtypeStruct((groups,) + tile, parts.dtype),
        in_specs=[VMEM],
        out_specs=VMEM,
        scratch_shapes=[
            pltpu.VMEM((toks,) + tile, parts.dtype),
            pltpu.VMEM((toks,) + tile, parts.dtype),
            pltpu.VMEM((max(ranks - 1, 1), groups) + tile, parts.dtype),
            pltpu.SemaphoreType.DMA((2, copies)),
        ],
        compiler_params=pltpu.CompilerParams(
            collective_id=number, has_side_effects=True, vmem_limit_bytes=40 * 1024 * 1024
        ),
    )(parts)


def shards(
    hidden,
    queries,
    cache,
    cache_lengths,
    wkv,
    wo,
    attn_gain,
    moe_gain,
    w_gate,
    w_up,
    w_down,
    expert_ids,
    gates,
):
    full_rows = lax.all_gather(hidden, "mdl", axis=1, tiled=True)
    span_len = full_rows.shape[0]
    toks = lax.axis_size("tok")
    core_count = lax.axis_size("mdl")
    ranks = toks // EXPERTS
    core_rows = span_len // core_count
    core_start = lax.axis_index("mdl") * core_rows
    own_rows = lax.dynamic_slice_in_dim(full_rows, core_start, core_rows, 0)
    normalized_input = rms_scale(own_rows, attn_gain).astype(jnp.bfloat16)
    kv_heads = wkv.shape[1]
    head_dim = wkv.shape[3]
    depth = wkv.shape[0]
    slices = normalized_input.reshape(core_rows, toks, depth).transpose(1, 0, 2)
    every_row = spread(slices, toks, 1, True, False, 1).reshape(-1, depth)
    partial_kv = jnp.dot(
        every_row, wkv.reshape(depth, -1), preferred_element_type=jnp.float32
    ).astype(jnp.bfloat16)
    terms = spread(partial_kv.reshape(toks, span_len, -1), toks, 1, False, False, 2)
    key_value_projection = jnp.sum(terms.astype(jnp.float32), axis=0).reshape(
        span_len, kv_heads, 2, head_dim
    )
    length = cache_lengths[0]
    positions = length + jnp.arange(span_len, dtype=jnp.int32)
    fresh_key_value = jnp.stack(
        [rotate(key_value_projection[:, :, 0], positions), key_value_projection[:, :, 1]], axis=2
    ).astype(jnp.bfloat16)
    head_group = queries.shape[1] // kv_heads
    outputs = []
    for head_index in range(kv_heads):
        query_rows = queries[:, head_index * head_group : (head_index + 1) * head_group].reshape(
            span_len * head_group, head_dim
        )
        attended = head_attention(
            query_rows,
            cache[0, :, head_index, 0],
            cache[0, :, head_index, 1],
            length,
            fresh_key_value[:, head_index, 0],
            fresh_key_value[:, head_index, 1],
            head_group,
        )
        outputs.append(attended.reshape(span_len, head_group * head_dim))
    heads_out = jnp.concatenate(outputs, axis=1)
    every_head = spread(heads_out, EXPERTS, ranks, False, True, 3)
    attn_part = jnp.dot(
        every_head.reshape(toks * span_len, -1),
        wo.reshape(-1, wo.shape[2]),
        preferred_element_type=jnp.float32,
    ).astype(jnp.bfloat16)
    attn_rows = collect(
        attn_part.reshape(toks, core_count, core_rows, -1), toks, 1, 4
    )
    attn_rows = attn_rows.transpose(1, 0, 2).reshape(core_rows, -1).astype(jnp.float32)
    resid = own_rows.astype(jnp.float32) + attn_rows
    moe_in = rms_scale(resid, moe_gain).astype(jnp.bfloat16)
    expert_range = jnp.arange(EXPERTS)
    matches = expert_ids[:, :, None] == expert_range[None, None, :]
    chosen = jnp.sum(matches.astype(jnp.int32), axis=1)
    route = jnp.sum(jnp.where(matches, gates[:, :, None], 0.0), axis=1)
    slot_of = jnp.cumsum(chosen, axis=0) - chosen
    capacity = core_rows * TOPK * 9 // (8 * EXPERTS)
    slot_range = jnp.arange(capacity)
    select = (slot_of.T[:, None, :] == slot_range[None, :, None]) & (chosen.T[:, None, :] > 0)
    send_rows = jnp.einsum(
        "eci,id->ecd", select.astype(jnp.bfloat16), moe_in, preferred_element_type=jnp.float32
    ).astype(jnp.bfloat16)
    model_width = moe_in.shape[1]
    received = spread(send_rows, EXPERTS, ranks, True, False, 5)
    flat_rows = received.reshape(-1, model_width)
    gate_val = jnp.dot(flat_rows, w_gate[0], preferred_element_type=jnp.float32)
    up_val = jnp.dot(flat_rows, w_up[0], preferred_element_type=jnp.float32)
    slab_hidden = (jax.nn.silu(gate_val) * up_val).astype(jnp.bfloat16)
    slab_out = jnp.dot(slab_hidden, w_down[0], preferred_element_type=jnp.float32).astype(
        jnp.bfloat16
    )
    summed = collect(slab_out.reshape(received.shape), EXPERTS, ranks, 6).astype(jnp.float32)
    weight_table = select.astype(jnp.float32) * route.T[:, None, :]
    moe_out = jnp.einsum("eci,ecd->id", weight_table, summed, precision=lax.Precision.HIGHEST)
    mixed = (resid + moe_out).astype(jnp.bfloat16)
    return (mixed, fresh_key_value)


def solution(mesh):
    in_specs = (
        P(("grp", "tok"), "mdl"),
        P(("grp", "tok"), "mdl", None),
        P(("grp", "tok"), None, "mdl", None, None),
        P(("grp", "tok")),
        P("tok", "mdl", None, None),
        P("mdl", None, "tok"),
        P(),
        P(),
        P(("tok", "mdl"), None, None),
        P(("tok", "mdl"), None, None),
        P(("tok", "mdl"), None, None),
        P(("grp", "tok", "mdl"), None),
        P(("grp", "tok", "mdl"), None),
    )
    out_specs = (P(("grp", "tok", "mdl"), None), P(("grp", "tok"), "mdl", None, None))
    return jax.shard_map(shards, mesh=mesh, in_specs=in_specs, out_specs=out_specs, check_vma=False)
```

```python
import functools
import math

import jax
import jax.numpy as jnp
from jax import lax
from jax.experimental import pallas as pl
from jax.experimental.pallas import tpu as pltpu
from jax.sharding import PartitionSpec as P

EXPERTS = 4
TOPK = 2


eps_norm = 1e-05
rope_base = 1000000.0
mask_fill = -1e30


def rms_scale(values_in, gain):
    values = values_in.astype(jnp.float32)
    meansq = jnp.mean(values * values, axis=-1, keepdims=True)
    return values * lax.rsqrt(meansq + eps_norm) * gain.astype(jnp.float32)


def rotate(key_rows, positions):
    half_dim = key_rows.shape[-1] // 2
    inverse = jnp.exp(
        jnp.arange(half_dim, dtype=jnp.float32) * (-2.0 * math.log(rope_base) / key_rows.shape[-1])
    )
    angle = positions.astype(jnp.float32)[:, None] * inverse[None, :]
    cosine = jnp.cos(angle)[:, None, :]
    sine_vals = jnp.sin(angle)[:, None, :]
    front_half = key_rows[..., :half_dim]
    back_half = key_rows[..., half_dim:]
    return jnp.concatenate(
        [front_half * cosine - back_half * sine_vals, back_half * cosine + front_half * sine_vals],
        axis=-1,
    )


def score_rows(query_rows, key_rows, scale_factor):
    return (
        lax.dot_general(
            query_rows, key_rows, (((1,), (1,)), ((), ())), preferred_element_type=jnp.float32
        )
        * scale_factor
    )


MESH = pl.DeviceIdType.MESH
VMEM = pl.BlockSpec(memory_space=pltpu.VMEM)


def place(tok, mdl):
    return (lax.axis_index("grp"), tok, mdl)


def greet(peers):
    barrier = pltpu.get_barrier_semaphore()
    for peer in peers:
        pl.semaphore_signal(barrier, inc=1, device_id=peer, device_id_type=MESH)
    pl.semaphore_wait(barrier, len(peers))


def peers_of(groups, ranks, cores):
    tok, mdl = lax.axis_index("tok"), lax.axis_index("mdl")
    group, rank = tok // ranks, tok % ranks
    peers = [place((group + d) % groups * ranks + rank, mdl) for d in range(1, groups)]
    peers += [place(group * ranks + (rank + d) % ranks, mdl) for d in range(1, ranks)]
    if cores:
        peers.append(place(tok, 1 - mdl))
    return peers


def remote(src, dst, sems, index, device):
    copy = pltpu.make_async_remote_copy(
        src_ref=src,
        dst_ref=dst,
        send_sem=sems.at[0, index],
        recv_sem=sems.at[1, index],
        device_id=device,
        device_id_type=MESH,
    )
    copy.start()
    return copy


def near_first(count):
    return sorted(range(1, count), key=lambda d: (min(d, count - d), d))


def cut(width, pieces):
    part = width // pieces
    return [pl.ds(c * part, part) for c in range(pieces)]


def spread_kernel(groups, ranks, cores, same, pieces, send, out, sems, local_sem):
    tok, mdl = lax.axis_index("tok"), lax.axis_index("mdl")
    group, rank = tok // ranks, tok % ranks
    columns = cut(send.shape[-1], pieces)
    greet(peers_of(groups, ranks, cores))

    def piece(index, c):
        return send.at[:, columns[c]] if same else send.at[index, :, columns[c]]

    def slot(index, c):
        return out.at[index, mdl, :, columns[c]] if cores else out.at[index, :, columns[c]]

    started = []

    def go(src, dst, device):
        copy = remote(src, dst, sems, len(started), device)
        started.append(copy)
        return copy

    first, second, third = {}, [], []
    for c in range(pieces):
        for d in near_first(groups):
            there = (group + d) % groups
            first[c, d] = go(piece(there, c), slot(tok, c), place(there * ranks + rank, mdl))

    def onward(src, index, c):
        for d in near_first(ranks):
            there = group * ranks + (rank + d) % ranks
            second.append((d, index, c, go(src, slot(index, c), place(there, mdl))))

    def across(src, index, c):
        if cores:
            third.append(go(src, slot(index, c), place(tok, 1 - mdl)))

    for c in range(pieces):
        onward(piece(group, c), tok, c)
    for c in range(pieces):
        across(piece(group, c), tok, c)
    own = pltpu.make_async_copy(
        send if same else send.at[group], out.at[tok, mdl] if cores else out.at[tok], local_sem
    )
    own.start()
    for c in range(pieces):
        for d in near_first(groups):
            first[c, d].wait_recv()
            index = (group + groups - d) % groups * ranks + rank
            onward(slot(index, c), index, c)
            across(slot(index, c), index, c)
    for d, index, c, copy in second:
        copy.wait_recv()
        index = index // ranks * ranks + (rank + ranks - d) % ranks
        across(slot(index, c), index, c)
    for copy in third:
        copy.wait_recv()
    for copy in started:
        copy.wait_send()
    own.wait()


def spread(send, groups, ranks, cores, same, number, pieces=1):
    tiles = send.shape if same else send.shape[1:]
    toks = groups * ranks
    core_count = lax.axis_size("mdl") if cores else 1
    lead = (toks, core_count) if cores else (toks,)
    copies = pieces * (groups - 1 + groups * (ranks - 1) + (toks if cores else 0))
    return pl.pallas_call(
        functools.partial(spread_kernel, groups, ranks, cores, same, pieces),
        out_shape=jax.ShapeDtypeStruct(lead + tiles, send.dtype),
        in_specs=[VMEM],
        out_specs=VMEM,
        scratch_shapes=[pltpu.SemaphoreType.DMA((2, copies)), pltpu.SemaphoreType.DMA],
        compiler_params=pltpu.CompilerParams(
            collective_id=number, has_side_effects=True, vmem_limit_bytes=40 * 1024 * 1024
        ),
    )(send)


def collect_kernel(groups, ranks, pieces, parts, out, near, held, mid, sems):
    tok, mdl = lax.axis_index("tok"), lax.axis_index("mdl")
    group, rank = tok // ranks, tok % ranks
    columns = cut(parts.shape[-1], pieces)
    greet(peers_of(groups, ranks, True))
    started = []

    def go(src, dst, device):
        copy = remote(src, dst, sems, len(started), device)
        started.append(copy)
        return copy

    far = near_first(groups)[::-1] + [0]
    order = [(r, g) for r in near_first(ranks) + [0] for g in far]

    def index_of(r, g):
        return (group + g) % groups * ranks + (rank + r) % ranks

    across, second, last = {}, {}, []
    for c in range(pieces):
        for r, g in order:
            index = index_of(r, g)
            across[c, r, g] = go(
                parts.at[index, 1 - mdl, :, columns[c]],
                near.at[index, :, columns[c]],
                place(tok, 1 - mdl),
            )

    def both_cores(c, r, g):
        index = index_of(r, g)
        across[c, r, g].wait_recv()
        return parts[index, mdl, :, columns[c]].astype(jnp.float32) + near[
            index, :, columns[c]
        ].astype(jnp.float32)

    def to_ranks(c):
        for r, g in order:
            if r == 0:
                continue
            index = index_of(r, g)
            held[index, :, columns[c]] = both_cores(c, r, g).astype(held.dtype)
            second[c, r, g] = go(
                held.at[index, :, columns[c]],
                mid.at[r - 1, g, :, columns[c]],
                place(group * ranks + (rank + r) % ranks, mdl),
            )

    def to_sources(c):
        for g in far:
            index = index_of(0, g)
            total = both_cores(c, 0, g)
            for r in range(1, ranks):
                second[c, r, g].wait_recv()
                total = total + mid[r - 1, g, :, columns[c]].astype(jnp.float32)
            if g == 0:
                out[group, :, columns[c]] = total.astype(out.dtype)
            else:
                held[index, :, columns[c]] = total.astype(held.dtype)
                last.append(
                    go(
                        held.at[index, :, columns[c]],
                        out.at[group, :, columns[c]],
                        place((group + g) % groups * ranks + rank, mdl),
                    )
                )

    for c in range(pieces + 1):
        if c < pieces:
            to_ranks(c)
        if c > 0:
            to_sources(c - 1)
    for copy in last:
        copy.wait_recv()
    for copy in started:
        copy.wait_send()


def collect(parts, groups, ranks, number, pieces=1):
    toks = groups * ranks
    tile = parts.shape[2:]
    copies = pieces * (toks + groups * (ranks - 1) + groups - 1)
    return pl.pallas_call(
        functools.partial(collect_kernel, groups, ranks, pieces),
        out_shape=jax.ShapeDtypeStruct((groups,) + tile, parts.dtype),
        in_specs=[VMEM],
        out_specs=VMEM,
        scratch_shapes=[
            pltpu.VMEM((toks,) + tile, parts.dtype),
            pltpu.VMEM((toks,) + tile, parts.dtype),
            pltpu.VMEM((max(ranks - 1, 1), groups) + tile, parts.dtype),
            pltpu.SemaphoreType.DMA((2, copies)),
        ],
        compiler_params=pltpu.CompilerParams(
            collective_id=number, has_side_effects=True, vmem_limit_bytes=40 * 1024 * 1024
        ),
    )(parts)


def attention_kernel(length, queries, cached, fresh, out):
    heads, span, width = queries.shape
    rows = heads * span
    query_rows = queries[...].reshape(rows, width)
    scale_factor = 1.0 / math.sqrt(width)
    limit = cached.shape[2]
    block = min(512, limit)
    token = lax.broadcasted_iota(jnp.int32, (rows, span), 0) % span
    column = lax.broadcasted_iota(jnp.int32, (rows, span), 1)
    scores = [
        jnp.where(
            column <= token, score_rows(query_rows, fresh[0, 0], scale_factor), mask_fill
        )
    ]
    values = [fresh[0, 1]]
    for start in range(0, limit, block):
        position = lax.broadcasted_iota(jnp.int32, (rows, block), 1) + start
        found = score_rows(query_rows, cached[0, 0, pl.ds(start, block)], scale_factor)
        scores.append(jnp.where(position < length[0], found, mask_fill))
        values.append(cached[0, 1, pl.ds(start, block)])
    top = functools.reduce(jnp.maximum, [jnp.max(x, axis=1, keepdims=True) for x in scores])
    total = jnp.zeros((rows, 1), jnp.float32)
    mixed = jnp.zeros((rows, width), jnp.float32)
    for found, value_rows in zip(scores, values):
        weights = jnp.exp(found - top)
        total += jnp.sum(weights, axis=1, keepdims=True)
        mixed += jnp.dot(
            weights.astype(jnp.bfloat16), value_rows, preferred_element_type=jnp.float32
        )
    attended = (mixed / total).astype(out.dtype)
    for head in range(heads):
        out[:, head * width : (head + 1) * width] = attended[head * span : (head + 1) * span]


def attention(queries, cache, lengths, fresh):
    span, query_heads, width = queries.shape
    kv_heads = cache.shape[2]
    per_head = query_heads // kv_heads
    limit = cache.shape[1]
    return pl.pallas_call(
        attention_kernel,
        grid=(kv_heads,),
        out_shape=jax.ShapeDtypeStruct((span, query_heads * width), jnp.bfloat16),
        in_specs=[
            pl.BlockSpec(memory_space=pltpu.SMEM),
            pl.BlockSpec((per_head, span, width), lambda h: (h, 0, 0)),
            pl.BlockSpec((1, 2, limit, width), lambda h: (h, 0, 0, 0)),
            pl.BlockSpec((1, 2, span, width), lambda h: (h, 0, 0, 0)),
        ],
        out_specs=pl.BlockSpec((span, per_head * width), lambda h: (0, h)),
        compiler_params=pltpu.CompilerParams(vmem_limit_bytes=40 * 1024 * 1024),
    )(
        lengths,
        queries.transpose(1, 0, 2),
        cache[0].transpose(1, 2, 0, 3),
        fresh.transpose(1, 2, 0, 3),
    )


def shards(
    hidden,
    queries,
    cache,
    cache_lengths,
    wkv,
    wo,
    attn_gain,
    moe_gain,
    w_gate,
    w_up,
    w_down,
    expert_ids,
    gates,
):
    full_rows = lax.all_gather(hidden, "mdl", axis=1, tiled=True)
    span_len = full_rows.shape[0]
    toks = lax.axis_size("tok")
    core_count = lax.axis_size("mdl")
    ranks = toks // EXPERTS
    core_rows = span_len // core_count
    core_start = lax.axis_index("mdl") * core_rows
    own_rows = lax.dynamic_slice_in_dim(full_rows, core_start, core_rows, 0)
    normalized_input = rms_scale(own_rows, attn_gain).astype(jnp.bfloat16)
    kv_heads = wkv.shape[1]
    head_dim = wkv.shape[3]
    depth = wkv.shape[0]
    slices = normalized_input.reshape(core_rows, toks, depth).transpose(1, 0, 2)
    every_row = spread(slices, toks, 1, True, False, 1).reshape(-1, depth)
    partial_kv = jnp.dot(
        every_row, wkv.reshape(depth, -1), preferred_element_type=jnp.float32
    ).astype(jnp.bfloat16)
    terms = spread(partial_kv.reshape(toks, span_len, -1), toks, 1, False, False, 2)
    key_value_projection = jnp.sum(terms.astype(jnp.float32), axis=0).reshape(
        span_len, kv_heads, 2, head_dim
    )
    length = cache_lengths[0]
    positions = length + jnp.arange(span_len, dtype=jnp.int32)
    fresh_key_value = jnp.stack(
        [rotate(key_value_projection[:, :, 0], positions), key_value_projection[:, :, 1]], axis=2
    ).astype(jnp.bfloat16)
    heads_out = attention(queries, cache, cache_lengths, fresh_key_value)
    every_head = spread(heads_out, EXPERTS, ranks, False, True, 3, 2)
    attn_part = jnp.dot(
        every_head.reshape(toks * span_len, -1),
        wo.reshape(-1, wo.shape[2]),
        preferred_element_type=jnp.float32,
    ).astype(jnp.bfloat16)
    attn_rows = collect(
        attn_part.reshape(toks, core_count, core_rows, -1), toks, 1, 4
    )
    attn_rows = attn_rows.transpose(1, 0, 2).reshape(core_rows, -1).astype(jnp.float32)
    resid = own_rows.astype(jnp.float32) + attn_rows
    moe_in = rms_scale(resid, moe_gain).astype(jnp.bfloat16)
    expert_range = jnp.arange(EXPERTS)
    matches = expert_ids[:, :, None] == expert_range[None, None, :]
    chosen = jnp.sum(matches.astype(jnp.int32), axis=1)
    route = jnp.sum(jnp.where(matches, gates[:, :, None], 0.0), axis=1)
    slot_of = jnp.cumsum(chosen, axis=0) - chosen
    capacity = core_rows * TOPK * 9 // (8 * EXPERTS)
    slot_range = jnp.arange(capacity)
    select = (slot_of.T[:, None, :] == slot_range[None, :, None]) & (chosen.T[:, None, :] > 0)
    send_rows = jnp.einsum(
        "eci,id->ecd", select.astype(jnp.bfloat16), moe_in, preferred_element_type=jnp.float32
    ).astype(jnp.bfloat16)
    model_width = moe_in.shape[1]
    received = spread(send_rows, EXPERTS, ranks, True, False, 5, 4)
    flat_rows = received.reshape(-1, model_width)
    gate_val = jnp.dot(flat_rows, w_gate[0], preferred_element_type=jnp.float32)
    up_val = jnp.dot(flat_rows, w_up[0], preferred_element_type=jnp.float32)
    slab_hidden = (jax.nn.silu(gate_val) * up_val).astype(jnp.bfloat16)
    slab_out = jnp.dot(slab_hidden, w_down[0], preferred_element_type=jnp.float32).astype(
        jnp.bfloat16
    )
    summed = collect(slab_out.reshape(received.shape), EXPERTS, ranks, 6, 4).astype(jnp.float32)
    weight_table = select.astype(jnp.float32) * route.T[:, None, :]
    moe_out = jnp.einsum("eci,ecd->id", weight_table, summed, precision=lax.Precision.HIGHEST)
    mixed = (resid + moe_out).astype(jnp.bfloat16)
    return (mixed, fresh_key_value)


def solution(mesh):
    in_specs = (
        P(("grp", "tok"), "mdl"),
        P(("grp", "tok"), "mdl", None),
        P(("grp", "tok"), None, "mdl", None, None),
        P(("grp", "tok")),
        P("tok", "mdl", None, None),
        P("mdl", None, "tok"),
        P(),
        P(),
        P(("tok", "mdl"), None, None),
        P(("tok", "mdl"), None, None),
        P(("tok", "mdl"), None, None),
        P(("grp", "tok", "mdl"), None),
        P(("grp", "tok", "mdl"), None),
    )
    out_specs = (P(("grp", "tok", "mdl"), None), P(("grp", "tok"), "mdl", None, None))
    return jax.shard_map(shards, mesh=mesh, in_specs=in_specs, out_specs=out_specs, check_vma=False)
```
